256 devices in a mesh: tm: 8 (over z), height: 4 (over y), width: 8 (over x, core).
Axes of the slice: x: 4, y: 4, z: 8, core: 2. Of those that a mesh axis runs over, the one named last changes fastest.
Arguments:
- frames: bfloat16 [16, 64, 128, 384], P('tm', 'height', 'width'), may hold values from -20 to 20
- attn_gain: float32 [384], replicated, may hold values from 0.25 to 1.75
- qkv_weight: bfloat16 [384, 1152], replicated, may hold values from -2 to 2
- proj_weight: bfloat16 [384, 384], replicated, may hold values from -0.3125 to 0.3125
- proj_bias: float32 [384], replicated, may hold values from -1.5 to 1.5
- conv_gain: float32 [384], replicated, may hold values from 0.25 to 1.75
- conv_weight: bfloat16 [3, 3, 3, 384, 384], replicated, may hold values from -0.0625 to 0.0625
- conv_bias: float32 [384], replicated, may hold values from -1.5 to 1.5
Outputs:
- decoded: bfloat16 [16, 64, 128, 384], P('tm', 'height', 'width')
The draws below stay inside these ranges and needn't reach their ends.
All inputs are finite; a program needn't handle non-finite values.
Results may differ from the reference program's by a relative error of at most 0.011.
Values may be sent and summed in bfloat16 or wider, within the bound.
No kernel may reach another device: no remote copies, remote signals or barrier semaphores. Data moves between devices by JAX's collectives and lax.ppermute only.
A program may use at most 128 MiB of HBM per device.

```python
import math
import jax
import jax.numpy as jnp
from jax import lax

C = 384
FRAMES = 16
HEIGHT_CELLS = 64
WIDTH_CELLS = 128


def draw_frames(key, part):
    first = jax.random.fold_in(jax.random.fold_in(key, 11), 0)
    shape_all = (FRAMES, HEIGHT_CELLS, WIDTH_CELLS, C)
    base = jax.random.normal(first, shape_all, jnp.float32)
    return jnp.clip(base, -20.0, 20.0).astype(jnp.bfloat16)


def draw_qkv_weight(key, part):
    first = jax.random.fold_in(jax.random.fold_in(key, 23), 0)
    third = jax.random.fold_in(jax.random.fold_in(key, 23), 2)
    fourth = jax.random.fold_in(jax.random.fold_in(key, 23), 3)
    root_scale = C ** (-0.5)
    query_part = 1.6 * root_scale * jax.random.normal(first, (C, C), jnp.float32)
    key_part = 1.6 * root_scale * jax.random.normal(third, (C, C), jnp.float32)
    value_part = root_scale * jax.random.normal(fourth, (C, C), jnp.float32)
    return jnp.clip(jnp.concatenate([query_part, key_part, value_part], axis=1), -2.0, 2.0).astype(jnp.bfloat16)


def normal_values(key, extent, width, bound, held_as=jnp.bfloat16):
    values = width * jax.random.normal(key, extent, jnp.float32)
    return jnp.clip(values, min=-bound, max=bound).astype(held_as)


def setup_inputs(seed: int = 0) -> dict:
    arg_keys = jax.random.split(jax.random.key(seed), 9)
    return {
        "frames": draw_frames(jax.random.fold_in(arg_keys[8], 71), 0),
        "attn_gain": jnp.clip(1.0 + 0.15 * jax.random.normal(arg_keys[1], (C,), jnp.float32), 0.25, 1.75),
        "qkv_weight": draw_qkv_weight(jax.random.fold_in(arg_keys[8], 71), 0),
        "proj_weight": normal_values(arg_keys[3], (C, C), C ** -0.5, 0.3125),
        "proj_bias": normal_values(arg_keys[4], (C,), 0.3, 1.5, jnp.float32),
        "conv_gain": jnp.clip(1.0 + 0.15 * jax.random.normal(arg_keys[5], (C,), jnp.float32), 0.25, 1.75),
        "conv_weight": normal_values(arg_keys[6], (3, 3, 3, C, C), (27 * C) ** -0.5, 0.0625),
        "conv_bias": normal_values(arg_keys[7], (C,), 0.3, 1.5, jnp.float32),
    }


epsilon = 1e-06

def rms_scale(values, gain_row):
    widened = values.astype(jnp.float32)
    mean_square = lax.optimization_barrier(jnp.mean(widened * widened, axis=-1, keepdims=True))
    return widened * lax.rsqrt(mean_square + epsilon) * gain_row

def reference(frames, attn_gain, qkv_weight, proj_weight, proj_bias, conv_gain, conv_weight, conv_bias):
    frame_count, height_rows, width_cols, channels = frames.shape
    flattened = frames.reshape(frame_count, height_rows * width_cols, channels)
    attn_in = rms_scale(flattened, attn_gain).astype(jnp.bfloat16)
    score_scale = 1.0 / math.sqrt(channels)

    def one_frame(frame_in):
        projected = jnp.dot(frame_in, qkv_weight, preferred_element_type=jnp.float32).astype(jnp.bfloat16)
        queries = projected[:, :channels]
        key_block = projected[:, channels:2 * channels]
        value_block = projected[:, 2 * channels:]
        scores = jnp.dot(queries, key_block.T, preferred_element_type=jnp.float32) * score_scale
        row_max = lax.optimization_barrier(jnp.max(scores, axis=-1, keepdims=True))
        weights = jnp.exp(scores - row_max)
        row_sum = lax.optimization_barrier(jnp.sum(weights, axis=-1, keepdims=True))
        summed = jnp.dot(weights.astype(jnp.bfloat16), value_block, preferred_element_type=jnp.float32)
        return (summed / row_sum).astype(jnp.bfloat16)
    attended = lax.map(one_frame, attn_in)
    projected_out = jnp.dot(attended.reshape(-1, channels), proj_weight, preferred_element_type=jnp.float32)
    mixed = (flattened.reshape(-1, channels).astype(jnp.float32) + projected_out + proj_bias).astype(jnp.bfloat16)
    conv_in = jax.nn.silu(rms_scale(mixed, conv_gain)).astype(jnp.bfloat16)
    conv_in = conv_in.reshape(frame_count, height_rows, width_cols, channels)
    padded = jnp.pad(conv_in, ((2, 0), (1, 1), (1, 1), (0, 0)))
    conv_out = jnp.zeros((frame_count * height_rows * width_cols, channels), jnp.float32)
    for step_t in range(3):
        for step_h in range(3):
            for step_w in range(3):
                window = padded[step_t:step_t + frame_count, step_h:step_h + height_rows, step_w:step_w + width_cols]
                conv_out = conv_out + jnp.dot(window.reshape(-1, channels), conv_weight[step_t, step_h, step_w], preferred_element_type=jnp.float32)
    decoded = mixed.astype(jnp.float32) + conv_out + conv_bias
    return decoded.astype(jnp.bfloat16).reshape(frame_count, height_rows, width_cols, channels)
```

```python
import functools
import math

import jax
import jax.numpy as jnp
from jax import lax
from jax.experimental import pallas as pl
from jax.experimental.pallas import tpu as pltpu
from jax.sharding import Mesh
from jax.sharding import PartitionSpec as P

epsilon = 1e-06
C = 384
CELLS = 256
ROWS = 2 * CELLS
KEYS = 4 * ROWS
PACK = ROWS + 32
PLANE = ("height", "x", "core")
VM = pl.BlockSpec(memory_space=pltpu.VMEM)
SM = pl.BlockSpec(memory_space=pltpu.SMEM)
BF = jnp.bfloat16
F32 = jnp.float32


def kernel_call(body, outs, n_in, flops, scratch=(), specs=None, limit=20):
    return pl.pallas_call(
        body,
        out_shape=outs,
        in_specs=specs or [VM] * n_in,
        out_specs=jax.tree.map(lambda _: VM, outs),
        scratch_shapes=list(scratch),
        compiler_params=pltpu.CompilerParams(vmem_limit_bytes=limit << 20),
        cost_estimate=pl.CostEstimate(flops=flops, bytes_accessed=1 << 20, transcendentals=0),
    )


def normed(values, gain):
    mean_square = jnp.sum(values * values, axis=-1, keepdims=True) * (1.0 / C)
    return values * lax.rsqrt(mean_square + epsilon) * gain


def prepare(keep_ref, recv_ref, gain_ref, qkv_ref, y_ref, q_ref):
    gain = gain_ref[...]
    for part, ref in enumerate((keep_ref, recv_ref)):
        y_ref[part * CELLS : (part + 1) * CELLS, :] = normed(ref[...].astype(F32), gain).astype(BF)
    q = jnp.dot(y_ref[...], qkv_ref[:, :C], preferred_element_type=F32).astype(BF)
    folded = lax.dot_general(
        q, qkv_ref[:, C : 2 * C], (((1,), (1,)), ((), ())), preferred_element_type=F32
    )
    q_ref[...] = (folded * (math.log2(math.e) / math.sqrt(C))).astype(BF)


def attend(q_ref, k0_ref, k1_ref, k2_ref, k3_ref, out_ref, scores_ref):
    blocks = (k0_ref, k1_ref, k2_ref, k3_ref)
    q = q_ref[...]
    top = jnp.full((ROWS, 128), -jnp.inf, F32)
    for j, ref in enumerate(blocks):
        s = lax.dot_general(q, ref[...], (((1,), (1,)), ((), ())), preferred_element_type=F32)
        scores_ref[:, j * ROWS : (j + 1) * ROWS] = s
        for g in range(ROWS // 128):
            top = jnp.maximum(top, s[:, g * 128 : (g + 1) * 128])
    row_max = jnp.max(top, axis=-1, keepdims=True)
    total = jnp.zeros((ROWS, 128), F32)
    acc = None
    for j, ref in enumerate(blocks):
        w = jnp.exp2(scores_ref[:, j * ROWS : (j + 1) * ROWS] - row_max)
        for g in range(ROWS // 128):
            total = total + w[:, g * 128 : (g + 1) * 128]
        part = jnp.dot(w.astype(BF), ref[...], preferred_element_type=F32)
        acc = part if acc is None else acc + part
    row_sum = jnp.sum(total, axis=-1, keepdims=True)
    out_ref[:ROWS, :] = (acc / row_sum).astype(BF)
    lse = row_max + jnp.log2(row_sum)
    row = jnp.broadcast_to(lse, (ROWS, 128)).T[:16, :]
    high = row.astype(BF).astype(F32)
    rest = row - high
    middle = rest.astype(BF).astype(F32)
    low = rest - middle
    which = lax.broadcasted_iota(jnp.int32, (16, ROWS), 0)
    packed = jnp.where(which == 0, high, jnp.where(which == 1, middle, low)).astype(BF)
    out_ref[ROWS : ROWS + 16, :] = packed[:, :C]
    out_ref[ROWS + 16 :, :] = jnp.concatenate(
        [packed[:, C:], jnp.zeros((16, 2 * C - ROWS), BF)], axis=1
    )


def column_of(pack_ref):
    def summed(block):
        row = (block[0:1, :] + block[1:2, :]) + block[2:3, :]
        return jnp.broadcast_to(row, (128, row.shape[1])).T

    first = summed(pack_ref[ROWS : ROWS + 16, :].astype(F32))
    second = summed(pack_ref[ROWS + 16 :, : ROWS - C].astype(F32))
    return jnp.concatenate([first, second], axis=0)[:, :1]


def merge(p0, p1, p2, p3, keep_ref, recv_ref, qkv_ref, proj_ref, bias_ref, mixed_ref, back_ref):
    packs = (p0, p1, p2, p3)
    lses = [column_of(p) for p in packs]
    top = jnp.maximum(jnp.maximum(lses[0], lses[1]), jnp.maximum(lses[2], lses[3]))
    shares = [jnp.exp2(v - top) for v in lses]
    inverse = 1.0 / ((shares[0] + shares[1]) + (shares[2] + shares[3]))
    total = None
    for p, share in zip(packs, shares):
        term = p[:ROWS, :].astype(F32) * (share * inverse)
        total = term if total is None else total + term
    attended = jnp.dot(total.astype(BF), qkv_ref[:, 2 * C :], preferred_element_type=F32)
    projected = jnp.dot(attended.astype(BF), proj_ref[...], preferred_element_type=F32)
    projected = projected + bias_ref[...]
    mixed_ref[...] = (keep_ref[...].astype(F32) + projected[:CELLS]).astype(BF)
    back_ref[...] = (recv_ref[...].astype(F32) + projected[CELLS:]).astype(BF)


def activate(core_ref, keep_ref, recv_ref, gain_ref, mixed_ref, conv_ref):
    core = core_ref[0]
    gain = gain_ref[...]
    for ref, place in ((keep_ref, core), (recv_ref, 1 - core)):
        start = pl.multiple_of(place * CELLS, CELLS)
        value = ref[...]
        mixed_ref[pl.ds(start, CELLS), :] = value
        v = normed(value.astype(F32), gain)
        conv_ref[pl.ds(start, CELLS), :] = (v / (1.0 + jnp.exp(-v))).astype(BF)


def spread(x_ref, rows_ref, cols_ref, pads_ref):
    for f in range(2):
        pads_ref[1, f, 0:16, :] = rows_ref[0, f]
        pads_ref[1, f, 16:272, :] = x_ref[f]
        pads_ref[1, f, 272:288, :] = rows_ref[1, f]
        center = pads_ref[1, f].astype(F32)
        place = lax.broadcasted_iota(jnp.int32, (288, C), 0) % 16
        for c, amount, edge in ((0, 1, 0), (2, 287, 15)):
            moved = pltpu.roll(center, amount, 0)
            side = cols_ref[c // 2, f].astype(F32)
            side = jnp.broadcast_to(side[:, None, :], (18, 16, C)).reshape(288, C)
            pads_ref[c, f] = jnp.where(place == edge, side, moved).astype(BF)


def windows(pads_ref, f):
    return jnp.concatenate(
        [pads_ref[c, f, b * 16 : b * 16 + CELLS, :] for b in range(3) for c in range(3)], axis=1
    )


def convolve_own(x_ref, rows_ref, cols_ref, w1_ref, w2_ref, out_ref, pads_ref):
    spread(x_ref, rows_ref, cols_ref, pads_ref)
    first, second = windows(pads_ref, 0), windows(pads_ref, 1)
    out_ref[0] = jnp.dot(first, w2_ref[...], preferred_element_type=F32)
    out_ref[1] = jnp.dot(second, w2_ref[...], preferred_element_type=F32) + jnp.dot(
        first, w1_ref[...], preferred_element_type=F32
    )


def convolve_earlier(
    x_ref, rows_ref, cols_ref, w0_ref, w1_ref, own_ref, mixed_ref, bias_ref, out_ref, pads_ref
):
    spread(x_ref, rows_ref, cols_ref, pads_ref)
    first, second = windows(pads_ref, 0), windows(pads_ref, 1)
    base = [own_ref[f] + mixed_ref[f].astype(F32) + bias_ref[...] for f in range(2)]
    out_ref[0] = (
        jnp.dot(first, w0_ref[...], preferred_element_type=F32)
        + jnp.dot(second, w1_ref[...], preferred_element_type=F32)
        + base[0]
    ).astype(BF)
    out_ref[1] = (jnp.dot(second, w0_ref[...], preferred_element_type=F32) + base[1]).astype(BF)


def plane_pairs(move):
    pairs = []
    for y in range(4):
        for x in range(4):
            for c in range(2):
                ty, tx, tc = move(y, x, c)
                pairs.append(((y * 4 + x) * 2 + c, (ty * 4 + tx) * 2 + tc))
    return pairs


def along(by, swapped):
    def move(y, x, c):
        if (c == 1) != swapped:
            return (y + by) % 4, x, c
        return y, (x + by) % 4, c

    return plane_pairs(move)


def line_pairs(count, by):
    return [(i, i + by) for i in range(count) if 0 <= i + by < count]


def shards(
    frames, attn_gain, qkv_weight, proj_weight, proj_bias, conv_gain, conv_weight, conv_bias
):
    shape = jax.ShapeDtypeStruct
    core = lax.axis_index("core")
    tiles = frames.reshape(2, CELLS, C)
    keep = lax.dynamic_index_in_dim(tiles, core, 0, keepdims=False)
    send = lax.dynamic_index_in_dim(tiles, 1 - core, 0, keepdims=False)
    swap = plane_pairs(lambda y, x, c: (y, x, 1 - c))
    recv = lax.ppermute(send, PLANE, swap)

    y, q = kernel_call(
        prepare, (shape((ROWS, C), BF), shape((ROWS, C), BF)), 4, 4 * ROWS * C * C
    )(keep, recv, attn_gain.reshape(1, C), qkv_weight)
    keys = [y] + [lax.ppermute(y, PLANE, along(by, True)) for by in (1, -1, 2)]
    queries = [q] + [lax.ppermute(q, PLANE, along(by, False)) for by in (1, -1, 2)]
    attention = kernel_call(
        attend,
        shape((PACK, C), BF),
        5,
        4 * ROWS * KEYS * C,
        [pltpu.VMEM((ROWS, KEYS), F32)],
        limit=32,
    )
    packs = [attention(queries[0], *keys)]
    for place, by in ((1, -1), (2, 1), (3, 2)):
        packs.append(lax.ppermute(attention(queries[place], *keys), PLANE, along(by, False)))
    mixed_keep, mixed_back = kernel_call(
        merge, (shape((CELLS, C), BF), shape((CELLS, C), BF)), 9, 4 * ROWS * C * C
    )(*packs, keep, recv, qkv_weight, proj_weight, proj_bias.reshape(1, C))
    mixed_recv = lax.ppermute(mixed_back, PLANE, swap)
    mixed, conv_in = kernel_call(
        activate,
        (shape((2 * CELLS, C), BF), shape((2 * CELLS, C), BF)),
        4,
        1 << 20,
        specs=[SM, VM, VM, VM],
    )(core.astype(jnp.int32).reshape(1), mixed_keep, mixed_recv, conv_gain.reshape(1, C))
    mixed = mixed.reshape(2, CELLS, C)

    inner = conv_in.reshape(2, 16, 16, C)
    ahead = line_pairs(lax.axis_size("tm"), 1)
    earlier = lax.ppermute(conv_in, "tm", ahead)
    down, up = line_pairs(4, 1), line_pairs(4, -1)
    rows = jnp.stack(
        [
            lax.ppermute(inner[:, 15], "height", down),
            lax.ppermute(inner[:, 0], "height", up),
        ]
    )
    ends = [
        jnp.concatenate([rows[0][:, None, w], inner[:, :, w], rows[1][:, None, w]], axis=1)
        for w in (15, 0)
    ]
    right, left = line_pairs(8, 1), line_pairs(8, -1)
    cols = jnp.stack(
        [
            lax.ppermute(ends[0], ("x", "core"), right),
            lax.ppermute(ends[1], ("x", "core"), left),
        ]
    )
    edge = jnp.concatenate([rows.reshape(-1, C), cols.reshape(-1, C)], axis=0)
    edge = lax.ppermute(edge, "tm", ahead)
    early_rows = edge[: 4 * 16].reshape(2, 2, 16, C)
    early_cols = edge[4 * 16 :].reshape(2, 2, 18, C)

    w = conv_weight.reshape(3, 9 * C, C)
    pads = [pltpu.VMEM((3, 2, 288, C), BF)]
    own = kernel_call(
        convolve_own, shape((2, CELLS, C), F32), 5, 6 * CELLS * 9 * C * C, pads, limit=24
    )(conv_in.reshape(2, CELLS, C), rows, cols, w[1], w[2])
    decoded = kernel_call(
        convolve_earlier, shape((2, CELLS, C), BF), 8, 6 * CELLS * 9 * C * C, pads, limit=24
    )(
        earlier.reshape(2, CELLS, C),
        early_rows,
        early_cols,
        w[0],
        w[1],
        own,
        mixed,
        conv_bias.reshape(1, C),
    )
    return decoded.reshape(2, 16, 16, C)


def solution(mesh):
    inner = Mesh(mesh.devices.reshape(8, 4, 4, 2), ("tm", "height", "x", "core"))
    placed = P("tm", "height", ("x", "core"), None)
    in_specs = (placed, P(), P(), P(), P(), P(), P(), P())
    return jax.shard_map(
        shards, mesh=inner, in_specs=in_specs, out_specs=placed, check_vma=False
    )
```
